32 devices in a mesh: lat: 4 (over x, core), lon: 8 (over z, y).
Axes of the slice: x: 2, y: 2, z: 4, core: 2. Of those that a mesh axis runs over, the one named last changes fastest.
Arguments:
- background: bfloat16 [16, 256, 2560], P('lat', 'lon'), may hold values from -6 to 6
- band_cols: int32 [16], P('lat'), may hold values from 20 to 256, as said below
- obs_col: int32 [16, 512], P('lat', 'lon'), may hold values from 0 to 255, as said below
- obs_lev: int32 [16, 512], P('lat', 'lon'), may hold values from 0 to 39
- obs_mask: int32 [16, 512], P('lat', 'lon'), may hold values from 0 to 1, as said below
- innov: float32 [16, 512], P('lat', 'lon'), may hold values from -9 to 9
- obs_var: float32 [16, 512], P('lat', 'lon'), may hold values from 0.25 to 2.5
Outputs:
- analysis: bfloat16 [16, 256, 2560], P('lat', 'lon')
The draws below stay inside these ranges and needn't reach their ends.
Inputs may be any that keep to these rules, and one draw needn't show every extreme that they name: Band 0 has 20 columns, band 16 // 2 has 160 columns and the last band 256; columns from band_cols on are padding. `obs_col`: slot i of a band lies in the columns from i // 64 * 32 to that plus 32 - 1. An observation in use lies below its band's band_cols. No column holds more than 4 observations in use, and some column of every band holds exactly 4. `obs_mask`: 1 marks an observation in use.
All inputs are finite; a program needn't handle non-finite values.
Results may differ from the reference program's by a relative error of at most 0.0061.
Values may be sent and summed in bfloat16 or wider, within the bound.
A program may use at most 128 MiB of HBM per device.

```python
import math
import jax
import jax.numpy as jnp
from jax import lax

K = 64
LEV = 40
OC = 4
RADIUS = 8
ITERS = 4
MINCOLS = 20
C_DEV = 32
NOB_DEV = 64
W = 256
BANDS = 16
NOBS = 512
N_LON = 8


def band_counts(key):
    band_index = jnp.arange(BANDS, dtype=jnp.int32)
    jitter = jax.random.randint(jax.random.fold_in(key, 11), (BANDS,), 0, 9)
    baseline = MINCOLS + (W - MINCOLS) * band_index // (BANDS - 1)
    interior = (band_index > 0) & (band_index < BANDS - 1)
    counts = jnp.minimum(baseline + jnp.where(interior, jitter, 0), W)
    counts = jnp.where(band_index == BANDS // 2, W // 2 + C_DEV, counts)
    return counts.astype(jnp.int32)


def obs_layout(key):
    lengths = band_counts(key)
    capacity = C_DEV * OC
    block_total = BANDS * N_LON
    block_keys = jax.random.split(jax.random.fold_in(key, 23), block_total)

    def permute(sub_key):
        return jax.random.permutation(sub_key, capacity)
    orders = jax.vmap(permute)(block_keys)
    position = jnp.argsort(orders, axis=1)
    block_index = jnp.arange(block_total, dtype=jnp.int32)
    band_of = block_index // N_LON
    lane_of = block_index % N_LON
    upper = jnp.minimum(lengths, C_DEV)
    pinned_col = jax.random.randint(jax.random.fold_in(key, 31), (BANDS,), 0, upper)
    cell_col = jnp.arange(capacity, dtype=jnp.int32) // OC
    forced = (lane_of[:, None] == 0) & (cell_col[None, :] == pinned_col[band_of][:, None])
    priority = jnp.where(forced, -1, position)
    chosen = jnp.argsort(priority, axis=1, stable=True)[:, :NOB_DEV]
    column = lane_of[:, None] * C_DEV + chosen // OC
    draw_bits = jax.random.randint(jax.random.fold_in(key, 41), (block_total, NOB_DEV), 0, 8)
    kept = jnp.take_along_axis(forced, chosen, axis=1) | (column < lengths[band_of][:, None]) & (draw_bits > 0)
    return (column.reshape(BANDS, N_LON * NOB_DEV).astype(jnp.int32), kept.reshape(BANDS, N_LON * NOB_DEV).astype(jnp.int32))


def draw_band_cols(key, part):
    return band_counts(key)


def draw_obs_col(key, part):
    return obs_layout(key)[0]


def draw_obs_mask(key, part):
    return obs_layout(key)[1]


def touch_ends(array, stream_key, least, largest):
    longest = array.shape.index(max(array.shape))
    spots = []
    for shift in (0, 1):
        where = [jax.random.randint(jax.random.fold_in(stream_key, axis), (), 0, length) for axis, length in enumerate(array.shape)]
        where[longest] = (where[longest] + shift) % array.shape[longest]
        spots.append(tuple(where))
    return array.at[spots[0]].set(least).at[spots[1]].set(largest)


def block_levels(rng, extent, pieces, low, high):
    def one(dim, parts):
        steps = jax.random.uniform(jax.random.fold_in(jax.random.fold_in(rng, 6), dim), (parts,), jnp.float32, low / len(pieces), high / len(pieces))
        return jnp.repeat(jnp.exp(steps), extent[dim] // parts).reshape((-1,) + (1,) * (len(extent) - dim - 1))

    factor_of = one(*pieces[0])
    for cut in pieces[1:]:
        factor_of = factor_of * one(*cut)
    return factor_of


def centred(key, shape, scale, reach, cuts=(), held_as=jnp.bfloat16):
    gain = block_levels(key, shape, cuts, -0.22, 0.18) if cuts else 1.0
    values = jax.random.normal(key, shape, jnp.float32) * scale * gain
    return jnp.minimum(jnp.maximum(values, -reach), reach).astype(held_as)


def setup_inputs(seed: int = 0) -> dict:
    arg_keys = jax.random.split(jax.random.key(seed), 8)
    background = centred(arg_keys[0], (BANDS, W, LEV * K), 1.0, 6.0, ((0, 4), (1, 8)))
    band_cols = draw_band_cols(jax.random.fold_in(arg_keys[7], 71), 0)
    obs_col = draw_obs_col(jax.random.fold_in(arg_keys[7], 71), 0)
    obs_lev = touch_ends(jax.random.randint(arg_keys[3], (BANDS, NOBS), 0, LEV), jax.random.fold_in(arg_keys[3], 1), 0, LEV - 1).astype(jnp.int32)
    obs_mask = draw_obs_mask(jax.random.fold_in(arg_keys[7], 71), 0)
    innov = centred(arg_keys[5], (BANDS, NOBS), 1.5, 9.0, ((0, 4), (1, 8)), jnp.float32)
    obs_var = jnp.clip(jnp.exp(math.log(2.5) - 2.3025851 * jax.random.uniform(arg_keys[6], (BANDS, NOBS), jnp.float32) ** block_levels(arg_keys[6], (BANDS, NOBS), ((0, 4), (1, 8)), -0.2, 0.2)), 0.25, 2.5)
    return {"background": background, "band_cols": band_cols, "obs_col": obs_col, "obs_lev": obs_lev, "obs_mask": obs_mask, "innov": innov, "obs_var": obs_var}


EXACT_ARITHMETIC = lax.Precision.HIGHEST

def taper_weights(radius):
    half_width = radius / 2.0
    tapering = []
    for offset in range(1 - radius, radius):
        distance = abs(offset) / half_width
        if distance <= 1.0:
            weight = ((-0.25 * distance + 0.5) * distance + 0.625) * distance ** 3 - 5.0 / 3.0 * distance ** 2 + 1.0
        else:
            weight = (((distance / 12.0 - 0.5) * distance + 0.625) * distance + 5.0 / 3.0) * distance ** 2 - 5.0 * distance + 4.0 - 2.0 / (3.0 * distance)
        tapering.append(weight)
    return tapering

def centred_system(localized_weights, inflation):
    members = localized_weights.shape[-1]
    identity = jnp.eye(members, dtype=jnp.float32)
    row_mean = lax.optimization_barrier(jnp.mean(localized_weights, axis=-1))
    column_average = lax.optimization_barrier(jnp.mean(localized_weights, axis=-2))
    all_mean = lax.optimization_barrier(jnp.mean(row_mean, axis=-1))
    mean_shift = all_mean[..., None] - row_mean
    system = localized_weights - row_mean[..., :, None] - column_average[..., None, :] + all_mean[..., None, None] + (members - 1) / inflation * identity
    return (system, mean_shift)

def transform_of(system, mean_shift):
    members = system.shape[-1]
    identity = jnp.eye(members, dtype=jnp.float32)
    magnitude = jnp.sqrt(lax.optimization_barrier(jnp.sum(system * system, axis=(-2, -1))))
    root_est = system / magnitude[..., None, None]
    inv_root = jnp.broadcast_to(identity, system.shape)
    for iteration in range(ITERS):
        update = 1.5 * identity - 0.5 * jnp.einsum('...ij,...jk->...ik', inv_root, root_est, precision=EXACT_ARITHMETIC)
        if iteration + 1 < ITERS:
            root_est = jnp.einsum('...ij,...jk->...ik', root_est, update, precision=EXACT_ARITHMETIC)
        inv_root = jnp.einsum('...ij,...jk->...ik', update, inv_root, precision=EXACT_ARITHMETIC)
    half_step = jnp.einsum('...ij,...j->...i', inv_root, mean_shift, precision=EXACT_ARITHMETIC)
    mean_weight = jnp.einsum('...ij,...j->...i', inv_root, half_step, precision=EXACT_ARITHMETIC) / magnitude[..., None]
    scaling = jnp.sqrt(members - 1.0) / jnp.sqrt(magnitude)
    return inv_root * scaling[..., None, None] + mean_weight[..., :, None]

def reference(background, band_cols, obs_col, obs_lev, obs_mask, innov, obs_var):
    flattened = background.reshape(BANDS, W * LEV, K)
    row_index = (obs_col * LEV + obs_lev).astype(jnp.int32)
    picked = jnp.take_along_axis(flattened, row_index[:, :, None], axis=1).astype(jnp.float32)
    anomaly = picked - lax.optimization_barrier(jnp.mean(picked, axis=2, keepdims=True))
    mask_weight = obs_mask.astype(jnp.float32)
    obs_scale = jnp.sqrt(mask_weight / obs_var)
    depart = (obs_scale[:, :, None] * (anomaly - innov[:, :, None])).astype(jnp.bfloat16)
    depart_wide = depart.astype(jnp.float32)
    centre = lax.optimization_barrier(jnp.mean(depart_wide, axis=2, keepdims=True))
    spread = depart_wide - centre
    numerator = jnp.sum(centre * centre) + 1e-06
    denominator = jnp.sum(mask_weight) + jnp.sum(spread * spread) / (K - 1)
    inflation = numerator / denominator
    tapering = taper_weights(RADIUS)
    halo_width = RADIUS - 1
    positions = jnp.arange(W, dtype=jnp.int32)

    def one_band(band_item):
        ensemble, departures, columns_of, band_count = band_item
        outer_prod = departures[:, :, None] * departures[:, None, :]
        gram_table = jax.ops.segment_sum(outer_prod, columns_of, num_segments=W)
        localized_weights = jnp.zeros((W, K, K), jnp.float32)
        for tap_index in range(2 * halo_width + 1):
            wrapped_columns = jnp.mod(positions + (tap_index - halo_width), band_count).astype(jnp.int32)
            localized_weights = localized_weights + tapering[tap_index] * gram_table[wrapped_columns]
        system, mean_shift = centred_system(localized_weights, inflation)
        ensemble_transform = transform_of(system, mean_shift)
        field_values = ensemble.reshape(W, LEV, K).astype(jnp.float32)
        centred_ensemble_field = lax.optimization_barrier(jnp.mean(field_values, axis=2, keepdims=True))
        analysis_members = centred_ensemble_field + jnp.einsum('oqz,ozy->oqy', field_values - centred_ensemble_field, ensemble_transform, precision=EXACT_ARITHMETIC)
        analysis_members = jnp.where((positions < band_count)[:, None, None], analysis_members, 0.0)
        return analysis_members.reshape(W, LEV * K).astype(jnp.bfloat16)
    return lax.map(one_band, (background, depart_wide, obs_col, band_cols))
```

```python
import functools

import jax
import jax.numpy as jnp
from jax import lax
from jax.experimental import pallas as pl
from jax.experimental.pallas import tpu as pltpu
from jax.sharding import PartitionSpec as P

K = 64
LEV = 40
RADIUS = 8
ITERS = 4
GROUP = 4
LANES = 128
F32 = jnp.float32
BF16 = jnp.bfloat16
MESH = pl.DeviceIdType.MESH


def taper_weights(radius):
    half_width = radius / 2.0
    tapering = []
    for offset in range(radius):
        distance = offset / half_width
        if distance <= 1.0:
            weight = (
                ((-0.25 * distance + 0.5) * distance + 0.625) * distance**3
                - 5.0 / 3.0 * distance**2
                + 1.0
            )
        else:
            weight = (
                (((distance / 12.0 - 0.5) * distance + 0.625) * distance + 5.0 / 3.0) * distance**2
                - 5.0 * distance
                + 4.0
                - 2.0 / (3.0 * distance)
            )
        tapering.append(weight)
    return tapering


def dot(left, right):
    return jnp.dot(left, right, preferred_element_type=F32)


def iota(shape, dim):
    return lax.broadcasted_iota(jnp.int32, shape, dim)


def exchange_kernel(
    lats,
    lons,
    x_ref,
    col_ref,
    lev_ref,
    mask_ref,
    innov_ref,
    var_ref,
    pay_ref,
    shift_ref,
    stat_buf,
    pay_send,
    pay_recv,
    stat_send,
    stat_recv,
):
    total = lats * lons
    lat, lon = lax.axis_index("lat"), lax.axis_index("lon")
    me = lat * lons + lon
    barrier = pltpu.get_barrier_semaphore()

    def greet(step, carry):
        other = lax.rem(me + step, total)
        pl.semaphore_signal(
            barrier,
            inc=1,
            device_id=(other // lons, lax.rem(other, lons)),
            device_id_type=MESH,
        )
        return carry

    lax.fori_loop(1, total, greet, 0)

    bands, columns, width = x_ref.shape
    obs = col_ref.shape[1]
    half = obs // 2
    pairs = width // LANES
    local = (col_ref[...] - lon * columns).astype(F32)
    mask = mask_ref[...].astype(F32)
    scale = jnp.sqrt(mask / var_ref[...])
    params = jnp.concatenate([local, lev_ref[...].astype(F32), scale, innov_ref[...]], axis=0)
    params = jnp.concatenate([params, jnp.zeros((LANES - 4 * bands, obs), F32)], axis=0)
    params = jnp.concatenate([params, jnp.zeros((LANES, LANES - obs), F32)], axis=1)
    upright = jnp.transpose(params)[:obs]
    lane = iota((half, LANES), 1)
    col_ids = iota((obs, columns), 1)
    tags = jnp.zeros((half, LANES), F32)
    centre_sum = jnp.zeros((obs, 1), F32)
    spread_sum = jnp.zeros((obs, K), F32)
    for b in range(bands):
        col = upright[:, b : b + 1]
        lev = upright[:, bands + b : bands + b + 1].astype(jnp.int32)
        onehot = jnp.where(col_ids == col.astype(jnp.int32), 1.0, 0.0).astype(BF16)
        pair = lax.shift_right_logical(lev, 1)
        found = jnp.zeros((obs, LANES), F32)
        for p in range(pairs):
            got = dot(onehot, x_ref[b, :, p * LANES : (p + 1) * LANES])
            found = jnp.where(pair == p, got, found)
        picked = jnp.where((lev & 1) == 1, found[:, K:], found[:, :K])
        anomaly = picked - jnp.mean(picked, axis=1, keepdims=True)
        depart = upright[:, 2 * bands + b : 2 * bands + b + 1] * (
            anomaly - upright[:, 3 * bands + b : 3 * bands + b + 1]
        )
        depart = depart.astype(BF16).astype(F32)
        centre = jnp.mean(depart, axis=1, keepdims=True)
        spread = depart - centre
        centre_sum = centre_sum + centre * centre
        spread_sum = spread_sum + spread * spread
        packed = jnp.concatenate([depart[:half], depart[half:]], axis=1)
        pay_ref[lon, b * half : (b + 1) * half, :] = packed.astype(BF16)
        tags = jnp.where(lane == 2 * b, col[:half], tags)
        tags = jnp.where(lane == 2 * b + 1, col[half:], tags)
    pay_ref[lon, bands * half :, :] = tags.astype(BF16)
    numerator = jnp.sum(centre_sum, axis=0, keepdims=True)
    spread_row = jnp.sum(spread_sum, axis=0, keepdims=True)
    mask_row = jnp.sum(mask, axis=0, keepdims=True)
    denominator = jnp.sum(spread_row / (K - 1), axis=1, keepdims=True) + jnp.sum(
        mask_row, axis=1, keepdims=True
    )
    stat_lane = iota((8, LANES), 1)
    stat_buf[me] = jnp.where(stat_lane == 0, numerator, denominator)

    pl.semaphore_wait(barrier, total - 1)

    def stat_copy(slot, step, other):
        return pltpu.make_async_remote_copy(
            src_ref=stat_buf.at[slot],
            dst_ref=stat_buf.at[slot],
            send_sem=stat_send.at[step],
            recv_sem=stat_recv.at[slot],
            device_id=(other // lons, lax.rem(other, lons)),
            device_id_type=MESH,
        )

    def pay_copy(slot, step, other):
        return pltpu.make_async_remote_copy(
            src_ref=pay_ref.at[slot],
            dst_ref=pay_ref.at[slot],
            send_sem=pay_send.at[step],
            recv_sem=pay_recv.at[slot],
            device_id=(lat, other),
            device_id_type=MESH,
        )

    def send_stat(step, carry):
        stat_copy(me, step, lax.rem(me + step, total)).start()
        return carry

    def send_pay(step, carry):
        pay_copy(lon, step, lax.rem(lon + step, lons)).start()
        return carry

    lax.fori_loop(1, lons, send_pay, 0)
    lax.fori_loop(1, total, send_stat, 0)

    def take_stat(step, carry):
        stat_copy(me, step, lax.rem(me + step, total)).wait_send()
        source = lax.rem(me + total - step, total)
        stat_copy(source, step, source).wait_recv()
        return carry

    def take_pay(step, carry):
        pay_copy(lon, step, lax.rem(lon + step, lons)).wait_send()
        source = lax.rem(lon + lons - step, lons)
        pay_copy(source, step, source).wait_recv()
        return carry

    lax.fori_loop(1, total, take_stat, 0)
    lax.fori_loop(1, lons, take_pay, 0)
    stats = jnp.sum(stat_buf[...], axis=0)
    inflation = (stats[:, 0:1] + 1e-06) / stats[:, 1:2]
    shift_ref[...] = jnp.broadcast_to((K - 1) / inflation, (8, LANES))


def analysis_kernel(x_ref, pay_ref, shift_ref, cols_ref, out_ref, tags_s, xs, ys, w_s, st_s, rhs_s, gs):
    lon = lax.axis_index("lon")
    bands, columns, width = x_ref.shape
    lons, pay_rows, _ = pay_ref.shape
    half = pay_rows // (bands + 1)
    held = lons * half
    obs = 2 * held
    pairs = width // LANES
    groups = columns // GROUP
    span = GROUP * K
    tapering = taper_weights(RADIUS)
    tags = jnp.concatenate(
        [pay_ref[j, bands * half :, :] for j in range(lons)], axis=0
    ).astype(F32)
    tags_s[...] = jnp.transpose(tags)
    shift = shift_ref[0:1, 0:1]
    low = iota((K, LANES), 1) < K
    low_f = jnp.where(low, 1.0, 0.0)
    low_b = low_f.astype(BF16)
    high_b = (1.0 - low_f).astype(BF16)
    zero_b = jnp.zeros((K, LANES), BF16)
    eye = jnp.where(iota((K, span), 0) == iota((K, span), 1) % K, 1.0, 0.0)

    def block_diag(mat):
        left, right = mat[:, :LANES], mat[:, LANES:]
        return jnp.concatenate(
            [
                jnp.concatenate([left * low_b, zero_b], axis=1),
                jnp.concatenate([left * high_b, zero_b], axis=1),
                jnp.concatenate([zero_b, right * low_b], axis=1),
                jnp.concatenate([zero_b, right * high_b], axis=1),
            ],
            axis=0,
        )

    ones_bd = block_diag(jnp.ones((K, span), BF16))

    def one_band(b, carry):
        count = cols_ref[b]
        for p in range(pairs):
            xs[:, p, :] = x_ref[b, :, p * LANES : (p + 1) * LANES].astype(F32)
        start = pl.multiple_of(b * half, half)
        block = jnp.concatenate(
            [pay_ref[j, pl.ds(start, half), :] for j in range(lons)], axis=0
        ).astype(F32)
        turned = jnp.transpose(block)
        depart_t = jnp.concatenate([turned[:K], turned[K:]], axis=1)
        centre = jnp.mean(depart_t, axis=0, keepdims=True)
        st_s[...] = depart_t - centre
        rolled = pltpu.roll(block, K, 1)
        low_h = iota((held, LANES), 1) < K
        rhs = jnp.concatenate(
            [jnp.where(low_h, block, rolled), jnp.where(low_h, rolled, block)], axis=0
        )
        rhs_s[...] = (rhs - jnp.mean(rhs, axis=1, keepdims=True)).astype(BF16)
        col = jnp.concatenate(
            [tags_s[pl.ds(2 * b, 1), :], tags_s[pl.ds(2 * b + 1, 1), :]], axis=1
        )
        owner = (iota((1, obs), 1) % held) // half
        source = col.astype(jnp.int32) + owner * columns
        away = source - (lon * columns + iota((columns, obs), 0))
        away = jnp.where(2 * away > count, away - count, away)
        away = jnp.where(2 * away < -count, away + count, away)
        away = jnp.abs(away)
        weight = jnp.zeros((columns, obs), F32)
        for t in range(RADIUS):
            weight = jnp.where(away == t, tapering[t], weight)
        w_s[...] = weight
        mean_rows = dot((weight * -centre).astype(BF16), rhs_s[...])
        squares = []
        for g in range(groups):
            parts = []
            for c in range(g * GROUP, (g + 1) * GROUP):
                weighted = (st_s[...] * w_s[c : c + 1, :]).astype(BF16)
                parts.append(dot(weighted, rhs_s[...]))
            cat = jnp.concatenate(
                [jnp.where(low, parts[0], parts[1]), jnp.where(low, parts[2], parts[3])], axis=1
            )
            gs[g] = cat
            system = cat + shift * eye
            squares.append(jnp.sum(system * system, axis=0, keepdims=True))
        squares = jnp.concatenate(squares, axis=0)
        coarse = squares.astype(BF16)
        fine = (squares - coarse.astype(F32)).astype(BF16)
        sums = dot(jnp.concatenate([coarse, fine], axis=0), ones_bd)
        frob = jnp.sqrt(sums[:groups] + sums[groups:])
        inv_frob = 1.0 / frob
        scaling = jnp.sqrt((K - 1.0) * inv_frob)
        beta_all = 1.0 - shift * inv_frob
        batch = min(4, groups)
        for first in range(0, groups, batch):
            ids = range(first, first + batch)
            beta = [beta_all[g : g + 1] for g in ids]
            dev = [gs[g] * -inv_frob[g : g + 1] for g in ids]
            zeta = [1.0 + 0.5 * be for be in beta]
            root = [0.5 * d for d in dev]
            for it in range(ITERS):
                narrow = [d.astype(BF16) for d in dev]
                fixed = [block_diag(n) for n in narrow]
                if it == 0:
                    square = [dot(n, f) for n, f in zip(narrow, fixed)]
                elif it + 1 < ITERS:
                    both = [
                        dot(jnp.concatenate([n, r.astype(BF16)], axis=0), f)
                        for n, r, f in zip(narrow, root, fixed)
                    ]
                    square = [x[:K] for x in both]
                    prod = [x[K:] for x in both]
                else:
                    prod = [dot(r.astype(BF16), f) for r, f in zip(root, fixed)]
                if it > 0:
                    root = [
                        (1.0 + 0.5 * be) * r + (0.5 * ze) * d + 0.5 * x
                        for be, r, ze, d, x in zip(beta, root, zeta, dev, prod)
                    ]
                    zeta = [ze * (1.0 + 0.5 * be) for ze, be in zip(zeta, beta)]
                if it + 1 < ITERS:
                    square = [2.0 * be * d + s for be, d, s in zip(beta, dev, square)]
                    cube = [dot(s.astype(BF16), f) for s, f in zip(square, fixed)]
                    dev = [
                        (0.75 + 0.25 * be) * s + (0.25 * be * be) * d + 0.25 * c
                        for be, s, d, c in zip(beta, square, dev, cube)
                    ]
                    beta = [be * be * (0.75 + 0.25 * be) for be in beta]
            for i, g in enumerate(ids):
                c0 = g * GROUP
                row = jnp.concatenate(
                    [
                        jnp.where(low[:1], mean_rows[c0 : c0 + 1], mean_rows[c0 + 1 : c0 + 2]),
                        jnp.where(low[:1], mean_rows[c0 + 2 : c0 + 3], mean_rows[c0 + 3 : c0 + 4]),
                    ],
                    axis=1,
                )
                full = zeta[i] * eye + root[i]
                rows = jnp.broadcast_to(row, (8, span)).astype(BF16)
                half_step = zeta[i] * row + dot(rows, block_diag(root[i].astype(BF16)))[:1]
                shifted = dot((full * half_step).astype(BF16), ones_bd)
                scale = scaling[g : g + 1]
                mix = (
                    scale * full
                    + (1.0 - scale * zeta[i]) * (1.0 / K)
                    + shifted * inv_frob[g : g + 1]
                )
                for pair in range(GROUP // 2):
                    two = mix[:, pair * LANES : (pair + 1) * LANES]
                    swapped = pltpu.roll(two, K, 1).astype(BF16)
                    two = two.astype(BF16)
                    for side in range(2):
                        c = c0 + 2 * pair + side
                        upper, lower = (two, swapped) if side == 0 else (swapped, two)
                        apply = jnp.concatenate([upper * low_b, lower * high_b], axis=0)
                        ys[c] = dot(xs[c].astype(BF16), apply)
        keep = lon * columns + iota((columns, LANES), 0) < count
        for p in range(pairs):
            out_ref[b, :, p * LANES : (p + 1) * LANES] = jnp.where(
                keep, ys[:, p, :], 0.0
            ).astype(BF16)
        return carry

    lax.fori_loop(0, bands, one_band, 0)


def per_device(lats, lons, background, band_cols, obs_col, obs_lev, obs_mask, innov, obs_var):
    bands, columns, width = background.shape
    obs = obs_col.shape[1]
    half = obs // 2
    pay_rows = (bands + 1) * half
    total = lats * lons
    vmem = pl.BlockSpec(memory_space=pltpu.VMEM)
    pay, shift = pl.pallas_call(
        functools.partial(exchange_kernel, lats, lons),
        out_shape=(
            jax.ShapeDtypeStruct((lons, pay_rows, LANES), BF16),
            jax.ShapeDtypeStruct((8, LANES), F32),
        ),
        in_specs=[vmem] * 6,
        out_specs=(vmem, vmem),
        scratch_shapes=[
            pltpu.VMEM((total, 8, LANES), F32),
            pltpu.SemaphoreType.DMA((lons,)),
            pltpu.SemaphoreType.DMA((lons,)),
            pltpu.SemaphoreType.DMA((total,)),
            pltpu.SemaphoreType.DMA((total,)),
        ],
        compiler_params=pltpu.CompilerParams(collective_id=0, has_side_effects=True),
        name="exchange",
    )(background, obs_col, obs_lev, obs_mask, innov, obs_var)
    held = lons * half
    pairs = width // LANES
    return pl.pallas_call(
        analysis_kernel,
        out_shape=jax.ShapeDtypeStruct(background.shape, BF16),
        in_specs=[vmem, vmem, vmem, pl.BlockSpec(memory_space=pltpu.SMEM)],
        out_specs=vmem,
        scratch_shapes=[
            pltpu.VMEM((LANES, held), F32),
            pltpu.VMEM((columns, pairs, LANES), F32),
            pltpu.VMEM((columns, pairs, LANES), F32),
            pltpu.VMEM((columns, 2 * held), F32),
            pltpu.VMEM((K, 2 * held), F32),
            pltpu.VMEM((2 * held, LANES), BF16),
            pltpu.VMEM((columns // GROUP, K, GROUP * K), F32),
        ],
        name="analysis",
    )(background, pay, shift, band_cols)


def solution(mesh):
    placed = (P("lat", "lon", None), P("lat")) + (P("lat", "lon"),) * 5
    return jax.shard_map(
        functools.partial(per_device, mesh.shape["lat"], mesh.shape["lon"]),
        mesh=mesh,
        in_specs=placed,
        out_specs=P("lat", "lon", None),
        check_vma=False,
    )
```

```python
import functools

import jax
import jax.numpy as jnp
from jax import lax
from jax.experimental import pallas as pl
from jax.experimental.pallas import tpu as pltpu
from jax.sharding import PartitionSpec as P

K = 64
LEV = 40
RADIUS = 8
ITERS = 4
GROUP = 4
OC = 4
END_SLOTS = 32
FAR = 1 << 20
LANES = 128
F32 = jnp.float32
BF16 = jnp.bfloat16
MESH = pl.DeviceIdType.MESH


def taper_weights(radius):
    half_width = radius / 2.0
    tapering = []
    for offset in range(radius):
        distance = offset / half_width
        if distance <= 1.0:
            weight = (
                ((-0.25 * distance + 0.5) * distance + 0.625) * distance**3
                - 5.0 / 3.0 * distance**2
                + 1.0
            )
        else:
            weight = (
                (((distance / 12.0 - 0.5) * distance + 0.625) * distance + 5.0 / 3.0) * distance**2
                - 5.0 * distance
                + 4.0
                - 2.0 / (3.0 * distance)
            )
        tapering.append(weight)
    return tapering


def dot(left, right):
    return jnp.dot(left, right, preferred_element_type=F32)


def iota(shape, dim):
    return lax.broadcasted_iota(jnp.int32, shape, dim)


def exchange_kernel(
    lats,
    lons,
    x_ref,
    col_ref,
    lev_ref,
    mask_ref,
    innov_ref,
    var_ref,
    cols_ref,
    own_ref,
    side_ref,
    shift_ref,
    ends_buf,
    near_buf,
    tail_buf,
    lat_buf,
    lon_buf,
    near_send,
    near_recv,
    head_send,
    head_recv,
    tail_send,
    tail_recv,
    lat_send,
    lat_recv,
    lon_send,
    lon_recv,
):
    lat, lon = lax.axis_index("lat"), lax.axis_index("lon")
    barrier = pltpu.get_barrier_semaphore()
    near_buf[...] = jnp.zeros_like(near_buf)
    tail_buf[...] = jnp.zeros_like(tail_buf)

    def greet_lon(step, carry):
        pl.semaphore_signal(
            barrier, inc=1, device_id=(lat, lax.rem(lon + step, lons)), device_id_type=MESH
        )
        return carry

    def greet_lat(step, carry):
        pl.semaphore_signal(
            barrier, inc=1, device_id=(lax.rem(lat + step, lats), lon), device_id_type=MESH
        )
        return carry

    lax.fori_loop(1, lons, greet_lon, 0)
    lax.fori_loop(1, lats, greet_lat, 0)

    bands, columns, width = x_ref.shape
    obs = col_ref.shape[1]
    half = obs // 2
    pairs = width // LANES
    reach = RADIUS - 1
    ends = END_SLOTS
    first = lon * columns
    local_int = col_ref[...] - first
    local = local_int.astype(F32)
    mask = mask_ref[...].astype(F32)
    scale = jnp.sqrt(mask / var_ref[...])
    params = jnp.concatenate([local, lev_ref[...].astype(F32), scale, innov_ref[...]], axis=0)
    params = jnp.concatenate([params, jnp.zeros((LANES - 4 * bands, obs), F32)], axis=0)
    params = jnp.concatenate([params, jnp.zeros((LANES, LANES - obs), F32)], axis=1)
    upright = jnp.transpose(params)[:obs]
    col_ids = iota((obs, columns), 1)
    earlier = iota((obs, obs), 0) < iota((obs, obs), 1)
    slot_ids = iota((ends, obs), 0)
    centre_sum = jnp.zeros((obs, 1), F32)
    spread_sum = jnp.zeros((obs, K), F32)
    for b in range(bands):
        col = upright[:, b : b + 1]
        lev = upright[:, bands + b : bands + b + 1].astype(jnp.int32)
        onehot = jnp.where(col_ids == col.astype(jnp.int32), 1.0, 0.0).astype(BF16)
        pair = lax.shift_right_logical(lev, 1)
        found = jnp.zeros((obs, LANES), F32)
        for p in range(pairs):
            got = dot(onehot, x_ref[b, :, p * LANES : (p + 1) * LANES])
            found = jnp.where(pair == p, got, found)
        picked = jnp.where((lev & 1) == 1, found[:, K:], found[:, :K])
        anomaly = picked - jnp.mean(picked, axis=1, keepdims=True)
        depart_scale = upright[:, 2 * bands + b : 2 * bands + b + 1]
        depart = depart_scale * (anomaly - upright[:, 3 * bands + b : 3 * bands + b + 1])
        narrow = depart.astype(BF16)
        depart = narrow.astype(F32)
        centre = jnp.mean(depart, axis=1, keepdims=True)
        spread = depart - centre
        centre_sum = centre_sum + centre * centre
        spread_sum = spread_sum + spread * spread
        packed = jnp.concatenate([depart[:half], depart[half:]], axis=1)
        own_ref[b * half : (b + 1) * half, :] = packed.astype(BF16)
        row = local_int[b : b + 1]
        used = mask[b : b + 1] > 0.0
        same = (col == local[b : b + 1]) & (depart_scale > 0.0) & earlier
        rank = jnp.sum(jnp.where(same, 1.0, 0.0), axis=0, keepdims=True).astype(jnp.int32)
        bases = (row, row - (columns - reach), row + first - (cols_ref[b] - reach))
        marks = []
        for base in bases:
            fits = used & (base >= 0) & (base < reach)
            slot = jnp.where(fits, base * OC + rank, -1)
            marks.append(jnp.where(slot_ids == slot, 1.0, 0.0))
        compact = dot(jnp.concatenate(marks, axis=0).astype(BF16), narrow)
        for kind in range(3):
            low = kind * ends
            packed = jnp.concatenate(
                [compact[low : low + ends // 2], compact[low + ends // 2 : low + ends]], axis=1
            )
            ends_buf[kind, b * ends // 2 : (b + 1) * ends // 2, :] = packed.astype(BF16)
    numerator = jnp.sum(centre_sum, axis=0, keepdims=True)
    spread_row = jnp.sum(spread_sum, axis=0, keepdims=True)
    mask_row = jnp.sum(mask, axis=0, keepdims=True)
    denominator = jnp.sum(spread_row / (K - 1), axis=1, keepdims=True) + jnp.sum(
        mask_row, axis=1, keepdims=True
    )
    stat_lane = iota((8, LANES), 1)
    lat_buf[lat] = jnp.where(stat_lane == 0, numerator, denominator)

    pl.semaphore_wait(barrier, lons + lats - 2)

    def lat_copy(slot, step, other):
        return pltpu.make_async_remote_copy(
            src_ref=lat_buf.at[slot],
            dst_ref=lat_buf.at[slot],
            send_sem=lat_send.at[step],
            recv_sem=lat_recv.at[slot],
            device_id=(other, lon),
            device_id_type=MESH,
        )

    def lon_copy(slot, step, other):
        return pltpu.make_async_remote_copy(
            src_ref=lon_buf.at[slot],
            dst_ref=lon_buf.at[slot],
            send_sem=lon_send.at[step],
            recv_sem=lon_recv.at[slot],
            device_id=(lat, other),
            device_id_type=MESH,
        )

    def near_copy(kind, slot, other):
        return pltpu.make_async_remote_copy(
            src_ref=ends_buf.at[kind],
            dst_ref=near_buf.at[slot],
            send_sem=near_send.at[slot],
            recv_sem=near_recv.at[slot],
            device_id=(lat, other),
            device_id_type=MESH,
        )

    def head_copy(other):
        return pltpu.make_async_remote_copy(
            src_ref=ends_buf.at[0],
            dst_ref=near_buf.at[2],
            send_sem=head_send.at[other],
            recv_sem=head_recv,
            device_id=(lat, other),
            device_id_type=MESH,
        )

    def tail_copy(slot):
        return pltpu.make_async_remote_copy(
            src_ref=ends_buf.at[2],
            dst_ref=tail_buf.at[slot],
            send_sem=tail_send,
            recv_sem=tail_recv.at[slot],
            device_id=(lat, 0),
            device_id_type=MESH,
        )

    for step in range(1, lats):
        lat_copy(lat, step, lax.rem(lat + step, lats)).start()

    @pl.when(lon > 0)
    def _():
        tail_copy(lon).start()
        near_copy(0, 1, lon - 1).start()

    @pl.when(lon == 0)
    def _():
        def send(other, carry):
            head_copy(other).start()
            return carry

        lax.fori_loop(1, lons, send, 0)

    @pl.when(lon < lons - 1)
    def _():
        near_copy(1, 0, lon + 1).start()

    for step in range(1, lats):
        source = lax.rem(lat + lats - step, lats)
        lat_copy(source, step, source).wait_recv()
    lon_buf[lon] = jnp.sum(lat_buf[...], axis=0)

    def send_lon(step, carry):
        lon_copy(lon, step, lax.rem(lon + step, lons)).start()
        return carry

    lax.fori_loop(1, lons, send_lon, 0)
    for step in range(1, lats):
        lat_copy(lat, step, lax.rem(lat + step, lats)).wait_send()

    @pl.when(lon > 0)
    def _():
        near_copy(1, 0, lon - 1).wait_recv()
        head_copy(lon).wait_recv()
        tail_copy(lon).wait_send()
        near_copy(0, 1, lon - 1).wait_send()

    @pl.when(lon == 0)
    def _():
        def take(other, carry):
            head_copy(other).wait_send()
            tail_copy(other).wait_recv()
            return carry

        lax.fori_loop(1, lons, take, 0)

    @pl.when(lon < lons - 1)
    def _():
        near_copy(0, 1, lon + 1).wait_recv()
        near_copy(1, 0, lon + 1).wait_send()

    side_ref[0] = (
        near_buf[0].astype(F32) + jnp.sum(tail_buf[...].astype(F32), axis=0)
    ).astype(BF16)
    side_ref[1] = near_buf[1]
    side_ref[2] = near_buf[2]

    def take_lon(step, carry):
        lon_copy(lon, step, lax.rem(lon + step, lons)).wait_send()
        source = lax.rem(lon + lons - step, lons)
        lon_copy(source, step, source).wait_recv()
        return carry

    lax.fori_loop(1, lons, take_lon, 0)
    stats = jnp.sum(lon_buf[...], axis=0)
    inflation = (stats[:, 0:1] + 1e-06) / stats[:, 1:2]
    shift_ref[...] = jnp.broadcast_to((K - 1) / inflation, (8, LANES))


def analysis_kernel(
    x_ref, own_ref, side_ref, shift_ref, col_ref, cols_ref, out_ref, xs, ys, w_s, st_s, rhs_s, gs
):
    lon = lax.axis_index("lon")
    bands, columns, width = x_ref.shape
    half = own_ref.shape[0] // bands
    quarter = side_ref.shape[1] // bands
    held = LANES
    obs = 2 * held
    sides = half + 3 * quarter
    pairs = width // LANES
    groups = columns // GROUP
    span = GROUP * K
    tapering = taper_weights(RADIUS)
    shift = shift_ref[0:1, 0:1]
    low = iota((K, LANES), 1) < K
    low_f = jnp.where(low, 1.0, 0.0)
    low_b = low_f.astype(BF16)
    high_b = (1.0 - low_f).astype(BF16)
    zero_b = jnp.zeros((K, LANES), BF16)
    eye = jnp.where(iota((K, span), 0) == iota((K, span), 1) % K, 1.0, 0.0)

    def block_diag(mat):
        left, right = mat[:, :LANES], mat[:, LANES:]
        return jnp.concatenate(
            [
                jnp.concatenate([left * low_b, zero_b], axis=1),
                jnp.concatenate([left * high_b, zero_b], axis=1),
                jnp.concatenate([zero_b, right * low_b], axis=1),
                jnp.concatenate([zero_b, right * high_b], axis=1),
            ],
            axis=0,
        )

    ones_bd = block_diag(jnp.ones((K, span), BF16))

    def one_band(b, carry):
        count = cols_ref[b]
        for p in range(pairs):
            xs[:, p, :] = x_ref[b, :, p * LANES : (p + 1) * LANES].astype(F32)
        start = pl.multiple_of(b * half, half)
        side = pl.multiple_of(b * quarter, quarter)
        block = jnp.concatenate(
            [own_ref[pl.ds(start, half), :]]
            + [side_ref[kind, pl.ds(side, quarter), :] for kind in range(3)]
            + [jnp.zeros((held - sides, LANES), BF16)],
            axis=0,
        ).astype(F32)
        turned = jnp.transpose(block)
        depart_t = jnp.concatenate([turned[:K], turned[K:]], axis=1)
        centre = jnp.mean(depart_t, axis=0, keepdims=True)
        st_s[...] = depart_t - centre
        rolled = pltpu.roll(block, K, 1)
        low_h = iota((held, LANES), 1) < K
        rhs = jnp.concatenate(
            [jnp.where(low_h, block, rolled), jnp.where(low_h, rolled, block)], axis=0
        )
        rhs_s[...] = (rhs - jnp.mean(rhs, axis=1, keepdims=True)).astype(BF16)
        col = col_ref[pl.ds(b, 1), :] - lon * columns
        col = jnp.concatenate([col, jnp.zeros((1, held - 2 * half), jnp.int32)], axis=1)
        col = jnp.concatenate([col, jnp.roll(col, -half, axis=1)], axis=1)
        place = iota((1, obs), 1)
        spot = place % held
        slot = spot - half + (place // held) * quarter
        where_left = slot // OC - (RADIUS - 1)
        where_right = (slot - quarter) // OC + columns
        where_head = (slot - 2 * quarter) // OC + count - lon * columns
        source = jnp.where(
            spot < half,
            col,
            jnp.where(
                spot < half + quarter,
                where_left,
                jnp.where(
                    spot < half + 2 * quarter,
                    where_right,
                    jnp.where(spot < sides, where_head, FAR),
                ),
            ),
        )
        limit = jnp.where(spot < half, count, FAR)
        away = source - iota((columns, obs), 0)
        away = jnp.where(2 * away > limit, away - count, away)
        away = jnp.where(2 * away < -limit, away + count, away)
        away = jnp.abs(away)
        weight = jnp.zeros((columns, obs), F32)
        for t in range(RADIUS):
            weight = jnp.where(away == t, tapering[t], weight)
        w_s[...] = weight
        mean_rows = dot((weight * -centre).astype(BF16), rhs_s[...])
        squares = []
        for g in range(groups):
            parts = []
            for c in range(g * GROUP, (g + 1) * GROUP):
                weighted = (st_s[...] * w_s[c : c + 1, :]).astype(BF16)
                parts.append(dot(weighted, rhs_s[...]))
            cat = jnp.concatenate(
                [jnp.where(low, parts[0], parts[1]), jnp.where(low, parts[2], parts[3])], axis=1
            )
            gs[g] = cat
            system = cat + shift * eye
            squares.append(jnp.sum(system * system, axis=0, keepdims=True))
        squares = jnp.concatenate(squares, axis=0)
        coarse = squares.astype(BF16)
        fine = (squares - coarse.astype(F32)).astype(BF16)
        sums = dot(jnp.concatenate([coarse, fine], axis=0), ones_bd)
        frob = jnp.sqrt(sums[:groups] + sums[groups:])
        inv_frob = 1.0 / frob
        scaling = jnp.sqrt((K - 1.0) * inv_frob)
        beta_all = 1.0 - shift * inv_frob
        batch = min(4, groups)
        for first in range(0, groups, batch):
            ids = range(first, first + batch)
            beta = [beta_all[g : g + 1] for g in ids]
            dev = [gs[g] * -inv_frob[g : g + 1] for g in ids]
            zeta = [1.0 + 0.5 * be for be in beta]
            root = [0.5 * d for d in dev]
            for it in range(ITERS):
                narrow = [d.astype(BF16) for d in dev]
                fixed = [block_diag(n) for n in narrow]
                if it == 0:
                    square = [dot(n, f) for n, f in zip(narrow, fixed)]
                elif it + 1 < ITERS:
                    both = [
                        dot(jnp.concatenate([n, r.astype(BF16)], axis=0), f)
                        for n, r, f in zip(narrow, root, fixed)
                    ]
                    square = [x[:K] for x in both]
                    prod = [x[K:] for x in both]
                else:
                    prod = [dot(r.astype(BF16), f) for r, f in zip(root, fixed)]
                if it > 0:
                    root = [
                        (1.0 + 0.5 * be) * r + (0.5 * ze) * d + 0.5 * x
                        for be, r, ze, d, x in zip(beta, root, zeta, dev, prod)
                    ]
                    zeta = [ze * (1.0 + 0.5 * be) for ze, be in zip(zeta, beta)]
                if it + 1 < ITERS:
                    square = [2.0 * be * d + s for be, d, s in zip(beta, dev, square)]
                    cube = [dot(s.astype(BF16), f) for s, f in zip(square, fixed)]
                    dev = [
                        (0.75 + 0.25 * be) * s + (0.25 * be * be) * d + 0.25 * c
                        for be, s, d, c in zip(beta, square, dev, cube)
                    ]
                    beta = [be * be * (0.75 + 0.25 * be) for be in beta]
            for i, g in enumerate(ids):
                c0 = g * GROUP
                row = jnp.concatenate(
                    [
                        jnp.where(low[:1], mean_rows[c0 : c0 + 1], mean_rows[c0 + 1 : c0 + 2]),
                        jnp.where(low[:1], mean_rows[c0 + 2 : c0 + 3], mean_rows[c0 + 3 : c0 + 4]),
                    ],
                    axis=1,
                )
                full = zeta[i] * eye + root[i]
                rows = jnp.broadcast_to(row, (8, span)).astype(BF16)
                half_step = zeta[i] * row + dot(rows, block_diag(root[i].astype(BF16)))[:1]
                shifted = dot((full * half_step).astype(BF16), ones_bd)
                scale = scaling[g : g + 1]
                mix = (
                    scale * full
                    + (1.0 - scale * zeta[i]) * (1.0 / K)
                    + shifted * inv_frob[g : g + 1]
                )
                for pair in range(GROUP // 2):
                    two = mix[:, pair * LANES : (pair + 1) * LANES]
                    swapped = pltpu.roll(two, K, 1).astype(BF16)
                    two = two.astype(BF16)
                    for side in range(2):
                        c = c0 + 2 * pair + side
                        upper, lower = (two, swapped) if side == 0 else (swapped, two)
                        apply = jnp.concatenate([upper * low_b, lower * high_b], axis=0)
                        ys[c] = dot(xs[c].astype(BF16), apply)
        keep = lon * columns + iota((columns, LANES), 0) < count
        for p in range(pairs):
            out_ref[b, :, p * LANES : (p + 1) * LANES] = jnp.where(
                keep, ys[:, p, :], 0.0
            ).astype(BF16)
        return carry

    lax.fori_loop(0, bands, one_band, 0)


def per_device(lats, lons, background, band_cols, obs_col, obs_lev, obs_mask, innov, obs_var):
    bands, columns, width = background.shape
    obs = obs_col.shape[1]
    pairs = width // LANES
    vmem = pl.BlockSpec(memory_space=pltpu.VMEM)
    smem = pl.BlockSpec(memory_space=pltpu.SMEM)
    dma = pltpu.SemaphoreType.DMA
    end_rows = bands * END_SLOTS // 2
    own, side, shift = pl.pallas_call(
        functools.partial(exchange_kernel, lats, lons),
        out_shape=(
            jax.ShapeDtypeStruct((bands * obs // 2, LANES), BF16),
            jax.ShapeDtypeStruct((3, end_rows, LANES), BF16),
            jax.ShapeDtypeStruct((8, LANES), F32),
        ),
        in_specs=[vmem] * 6 + [smem],
        out_specs=(vmem, vmem, vmem),
        scratch_shapes=[
            pltpu.VMEM((3, end_rows, LANES), BF16),
            pltpu.VMEM((3, end_rows, LANES), BF16),
            pltpu.VMEM((lons, end_rows, LANES), BF16),
            pltpu.VMEM((lats, 8, LANES), F32),
            pltpu.VMEM((lons, 8, LANES), F32),
            dma((2,)),
            dma((2,)),
            dma((lons,)),
            dma,
            dma,
            dma((lons,)),
            dma((lats,)),
            dma((lats,)),
            dma((lons,)),
            dma((lons,)),
        ],
        compiler_params=pltpu.CompilerParams(collective_id=0, has_side_effects=True),
        name="exchange",
    )(background, obs_col, obs_lev, obs_mask, innov, obs_var, band_cols)
    return pl.pallas_call(
        analysis_kernel,
        out_shape=jax.ShapeDtypeStruct(background.shape, BF16),
        in_specs=[vmem] * 5 + [smem],
        out_specs=vmem,
        scratch_shapes=[
            pltpu.VMEM((columns, pairs, LANES), F32),
            pltpu.VMEM((columns, pairs, LANES), F32),
            pltpu.VMEM((columns, 2 * LANES), F32),
            pltpu.VMEM((K, 2 * LANES), F32),
            pltpu.VMEM((2 * LANES, LANES), BF16),
            pltpu.VMEM((columns // GROUP, K, GROUP * K), F32),
        ],
        name="analysis",
    )(background, own, side, shift, obs_col, band_cols)


def solution(mesh):
    placed = (P("lat", "lon", None), P("lat")) + (P("lat", "lon"),) * 5
    return jax.shard_map(
        functools.partial(per_device, mesh.shape["lat"], mesh.shape["lon"]),
        mesh=mesh,
        in_specs=placed,
        out_specs=P("lat", "lon", None),
        check_vma=False,
    )
```

```python
import functools

import jax
import jax.numpy as jnp
from jax import lax
from jax.experimental import pallas as pl
from jax.experimental.pallas import tpu as pltpu
from jax.sharding import PartitionSpec as P

K = 64
LEV = 40
RADIUS = 8
ITERS = 4
GROUP = 4
OC = 4
END_SLOTS = 32
FAR = 1 << 20
LANES = 128
F32 = jnp.float32
BF16 = jnp.bfloat16
MESH = pl.DeviceIdType.MESH


def taper_weights(radius):
    half_width = radius / 2.0
    tapering = []
    for offset in range(radius):
        distance = offset / half_width
        if distance <= 1.0:
            weight = (
                ((-0.25 * distance + 0.5) * distance + 0.625) * distance**3
                - 5.0 / 3.0 * distance**2
                + 1.0
            )
        else:
            weight = (
                (((distance / 12.0 - 0.5) * distance + 0.625) * distance + 5.0 / 3.0) * distance**2
                - 5.0 * distance
                + 4.0
                - 2.0 / (3.0 * distance)
            )
        tapering.append(weight)
    return tapering


def dot(left, right):
    return jnp.dot(left, right, preferred_element_type=F32)


def iota(shape, dim):
    return lax.broadcasted_iota(jnp.int32, shape, dim)


def exchange_kernel(
    lats,
    lons,
    x_ref,
    col_ref,
    lev_ref,
    mask_ref,
    innov_ref,
    var_ref,
    cols_ref,
    own_ref,
    side_ref,
    shift_ref,
    ends_buf,
    near_buf,
    tail_buf,
    lat_buf,
    lon_buf,
    near_send,
    near_recv,
    head_send,
    head_recv,
    tail_send,
    tail_recv,
    lat_send,
    lat_recv,
    lon_send,
    lon_recv,
):
    lat, lon = lax.axis_index("lat"), lax.axis_index("lon")
    barrier = pltpu.get_barrier_semaphore()
    near_buf[...] = jnp.zeros_like(near_buf)
    tail_buf[...] = jnp.zeros_like(tail_buf)

    def greet_lon(step, carry):
        pl.semaphore_signal(
            barrier, inc=1, device_id=(lat, lax.rem(lon + step, lons)), device_id_type=MESH
        )
        return carry

    def greet_lat(step, carry):
        pl.semaphore_signal(
            barrier, inc=1, device_id=(lax.rem(lat + step, lats), lon), device_id_type=MESH
        )
        return carry

    lax.fori_loop(1, lons, greet_lon, 0)
    lax.fori_loop(1, lats, greet_lat, 0)

    bands, columns, width = x_ref.shape
    obs = col_ref.shape[1]
    half = obs // 2
    pairs = width // LANES
    reach = RADIUS - 1
    ends = END_SLOTS
    first = lon * columns
    local_int = col_ref[...] - first
    local = local_int.astype(F32)
    mask = mask_ref[...].astype(F32)
    scale = jnp.sqrt(mask / var_ref[...])
    params = jnp.concatenate([local, lev_ref[...].astype(F32), scale, innov_ref[...]], axis=0)
    params = jnp.concatenate([params, jnp.zeros((LANES - 4 * bands, obs), F32)], axis=0)
    params = jnp.concatenate([params, jnp.zeros((LANES, LANES - obs), F32)], axis=1)
    upright = jnp.transpose(params)[:obs]
    col_ids = iota((obs, columns), 1)
    earlier = iota((obs, obs), 0) < iota((obs, obs), 1)
    slot_ids = iota((ends, obs), 0)
    centre_sum = jnp.zeros((obs, 1), F32)
    spread_sum = jnp.zeros((obs, K), F32)
    for b in range(bands):
        col = upright[:, b : b + 1]
        lev = upright[:, bands + b : bands + b + 1].astype(jnp.int32)
        onehot = jnp.where(col_ids == col.astype(jnp.int32), 1.0, 0.0).astype(BF16)
        pair = lax.shift_right_logical(lev, 1)
        found = jnp.zeros((obs, LANES), F32)
        for p in range(pairs):
            got = dot(onehot, x_ref[b, :, p * LANES : (p + 1) * LANES])
            found = jnp.where(pair == p, got, found)
        picked = jnp.where((lev & 1) == 1, found[:, K:], found[:, :K])
        anomaly = picked - jnp.mean(picked, axis=1, keepdims=True)
        depart_scale = upright[:, 2 * bands + b : 2 * bands + b + 1]
        depart = depart_scale * (anomaly - upright[:, 3 * bands + b : 3 * bands + b + 1])
        narrow = depart.astype(BF16)
        depart = narrow.astype(F32)
        centre = jnp.mean(depart, axis=1, keepdims=True)
        spread = depart - centre
        centre_sum = centre_sum + centre * centre
        spread_sum = spread_sum + spread * spread
        packed = jnp.concatenate([depart[:half], depart[half:]], axis=1)
        own_ref[b * half : (b + 1) * half, :] = packed.astype(BF16)
        row = local_int[b : b + 1]
        used = mask[b : b + 1] > 0.0
        same = (col == local[b : b + 1]) & (depart_scale > 0.0) & earlier
        rank = jnp.sum(jnp.where(same, 1.0, 0.0), axis=0, keepdims=True).astype(jnp.int32)
        bases = (row, row - (columns - reach), row + first - (cols_ref[b] - reach))
        marks = []
        for base in bases:
            fits = used & (base >= 0) & (base < reach)
            slot = jnp.where(fits, base * OC + rank, -1)
            marks.append(jnp.where(slot_ids == slot, 1.0, 0.0))
        compact = dot(jnp.concatenate(marks, axis=0).astype(BF16), narrow)
        for kind in range(3):
            low = kind * ends
            packed = jnp.concatenate(
                [compact[low : low + ends // 2], compact[low + ends // 2 : low + ends]], axis=1
            )
            ends_buf[kind, b * ends // 2 : (b + 1) * ends // 2, :] = packed.astype(BF16)
    numerator = jnp.sum(centre_sum, axis=0, keepdims=True)
    spread_row = jnp.sum(spread_sum, axis=0, keepdims=True)
    mask_row = jnp.sum(mask, axis=0, keepdims=True)
    denominator = jnp.sum(spread_row / (K - 1), axis=1, keepdims=True) + jnp.sum(
        mask_row, axis=1, keepdims=True
    )
    stat_lane = iota((8, LANES), 1)
    lat_buf[lat] = jnp.where(stat_lane == 0, numerator, denominator)

    pl.semaphore_wait(barrier, lons + lats - 2)

    def lat_copy(slot, step, other):
        return pltpu.make_async_remote_copy(
            src_ref=lat_buf.at[slot],
            dst_ref=lat_buf.at[slot],
            send_sem=lat_send.at[step],
            recv_sem=lat_recv.at[slot],
            device_id=(other, lon),
            device_id_type=MESH,
        )

    def lon_copy(slot, step, other):
        return pltpu.make_async_remote_copy(
            src_ref=lon_buf.at[slot],
            dst_ref=lon_buf.at[slot],
            send_sem=lon_send.at[step],
            recv_sem=lon_recv.at[slot],
            device_id=(lat, other),
            device_id_type=MESH,
        )

    def near_copy(kind, slot, other):
        return pltpu.make_async_remote_copy(
            src_ref=ends_buf.at[kind],
            dst_ref=near_buf.at[slot],
            send_sem=near_send.at[slot],
            recv_sem=near_recv.at[slot],
            device_id=(lat, other),
            device_id_type=MESH,
        )

    def head_copy(other):
        return pltpu.make_async_remote_copy(
            src_ref=ends_buf.at[0],
            dst_ref=near_buf.at[2],
            send_sem=head_send.at[other],
            recv_sem=head_recv,
            device_id=(lat, other),
            device_id_type=MESH,
        )

    def tail_copy(slot):
        return pltpu.make_async_remote_copy(
            src_ref=ends_buf.at[2],
            dst_ref=tail_buf.at[slot],
            send_sem=tail_send,
            recv_sem=tail_recv.at[slot],
            device_id=(lat, 0),
            device_id_type=MESH,
        )

    for step in range(1, lats):
        lat_copy(lat, step, lax.rem(lat + step, lats)).start()

    @pl.when(lon > 0)
    def _():
        tail_copy(lon).start()
        near_copy(0, 1, lon - 1).start()

    @pl.when(lon == 0)
    def _():
        def send(other, carry):
            head_copy(other).start()
            return carry

        lax.fori_loop(1, lons, send, 0)

    @pl.when(lon < lons - 1)
    def _():
        near_copy(1, 0, lon + 1).start()

    for step in range(1, lats):
        source = lax.rem(lat + lats - step, lats)
        lat_copy(source, step, source).wait_recv()
    lon_buf[lon] = jnp.sum(lat_buf[...], axis=0)

    def send_lon(step, carry):
        lon_copy(lon, step, lax.rem(lon + step, lons)).start()
        return carry

    lax.fori_loop(1, lons, send_lon, 0)
    for step in range(1, lats):
        lat_copy(lat, step, lax.rem(lat + step, lats)).wait_send()

    @pl.when(lon > 0)
    def _():
        near_copy(1, 0, lon - 1).wait_recv()
        head_copy(lon).wait_recv()
        tail_copy(lon).wait_send()
        near_copy(0, 1, lon - 1).wait_send()

    @pl.when(lon == 0)
    def _():
        def take(other, carry):
            head_copy(other).wait_send()
            tail_copy(other).wait_recv()
            return carry

        lax.fori_loop(1, lons, take, 0)

    @pl.when(lon < lons - 1)
    def _():
        near_copy(0, 1, lon + 1).wait_recv()
        near_copy(1, 0, lon + 1).wait_send()

    side_ref[0] = (
        near_buf[0].astype(F32) + jnp.sum(tail_buf[...].astype(F32), axis=0)
    ).astype(BF16)
    side_ref[1] = near_buf[1]
    side_ref[2] = near_buf[2]

    def take_lon(step, carry):
        lon_copy(lon, step, lax.rem(lon + step, lons)).wait_send()
        source = lax.rem(lon + lons - step, lons)
        lon_copy(source, step, source).wait_recv()
        return carry

    lax.fori_loop(1, lons, take_lon, 0)
    stats = jnp.sum(lon_buf[...], axis=0)
    inflation = (stats[:, 0:1] + 1e-06) / stats[:, 1:2]
    shift_ref[...] = jnp.broadcast_to((K - 1) / inflation, (8, LANES))


def analysis_kernel(
    x_ref, own_ref, side_ref, shift_ref, col_ref, cols_ref, out_ref, xs, ys, w_s, st_s, rhs_s, gs
):
    lon = lax.axis_index("lon")
    bands, columns, width = x_ref.shape
    half = own_ref.shape[0] // bands
    quarter = side_ref.shape[1] // bands
    held = LANES
    obs = 2 * held
    sides = half + 3 * quarter
    pairs = width // LANES
    groups = columns // GROUP
    span = GROUP * K
    tapering = taper_weights(RADIUS)
    shift = shift_ref[0:1, 0:1]
    low = iota((K, LANES), 1) < K
    low_f = jnp.where(low, 1.0, 0.0)
    low_b = low_f.astype(BF16)
    high_b = (1.0 - low_f).astype(BF16)
    zero_b = jnp.zeros((K, LANES), BF16)
    rows_x = xs.shape[0] // columns
    low_x = iota((rows_x, LANES), 1) < K
    eye = jnp.where(iota((K, span), 0) == iota((K, span), 1) % K, 1.0, 0.0)

    def block_diag(mat):
        left, right = mat[:, :LANES], mat[:, LANES:]
        return jnp.concatenate(
            [
                jnp.concatenate([left * low_b, zero_b], axis=1),
                jnp.concatenate([left * high_b, zero_b], axis=1),
                jnp.concatenate([zero_b, right * low_b], axis=1),
                jnp.concatenate([zero_b, right * high_b], axis=1),
            ],
            axis=0,
        )

    ones_bd = block_diag(jnp.ones((K, span), BF16))

    def one_band(b, carry):
        count = cols_ref[b]
        for p in range(pairs):
            strip = x_ref[b, :, p * LANES : (p + 1) * LANES].astype(F32)
            xs[pl.ds(p, columns, stride=rows_x), :] = strip
        start = pl.multiple_of(b * half, half)
        side = pl.multiple_of(b * quarter, quarter)
        block = jnp.concatenate(
            [own_ref[pl.ds(start, half), :]]
            + [side_ref[kind, pl.ds(side, quarter), :] for kind in range(3)]
            + [jnp.zeros((held - sides, LANES), BF16)],
            axis=0,
        ).astype(F32)
        turned = jnp.transpose(block)
        depart_t = jnp.concatenate([turned[:K], turned[K:]], axis=1)
        centre = jnp.mean(depart_t, axis=0, keepdims=True)
        st_s[...] = depart_t - centre
        rolled = pltpu.roll(block, K, 1)
        low_h = iota((held, LANES), 1) < K
        rhs = jnp.concatenate(
            [jnp.where(low_h, block, rolled), jnp.where(low_h, rolled, block)], axis=0
        )
        rhs_s[...] = (rhs - jnp.mean(rhs, axis=1, keepdims=True)).astype(BF16)
        col = col_ref[pl.ds(b, 1), :] - lon * columns
        col = jnp.concatenate([col, jnp.zeros((1, held - 2 * half), jnp.int32)], axis=1)
        col = jnp.concatenate([col, jnp.roll(col, -half, axis=1)], axis=1)
        place = iota((1, obs), 1)
        spot = place % held
        slot = spot - half + (place // held) * quarter
        where_left = slot // OC - (RADIUS - 1)
        where_right = (slot - quarter) // OC + columns
        where_head = (slot - 2 * quarter) // OC + count - lon * columns
        source = jnp.where(
            spot < half,
            col,
            jnp.where(
                spot < half + quarter,
                where_left,
                jnp.where(
                    spot < half + 2 * quarter,
                    where_right,
                    jnp.where(spot < sides, where_head, FAR),
                ),
            ),
        )
        limit = jnp.where(spot < half, count, FAR)
        away = source - iota((columns, obs), 0)
        away = jnp.where(2 * away > limit, away - count, away)
        away = jnp.where(2 * away < -limit, away + count, away)
        away = jnp.abs(away)
        weight = jnp.zeros((columns, obs), F32)
        for t in range(RADIUS):
            weight = jnp.where(away == t, tapering[t], weight)
        w_s[...] = weight
        mean_rows = dot((weight * -centre).astype(BF16), rhs_s[...])
        squares = []
        for g in range(groups):
            parts = []
            for c in range(g * GROUP, (g + 1) * GROUP):
                weighted = (st_s[...] * w_s[c : c + 1, :]).astype(BF16)
                parts.append(dot(weighted, rhs_s[...]))
            cat = jnp.concatenate(
                [jnp.where(low, parts[0], parts[1]), jnp.where(low, parts[2], parts[3])], axis=1
            )
            gs[g] = cat
            system = cat + shift * eye
            squares.append(jnp.sum(system * system, axis=0, keepdims=True))
        squares = jnp.concatenate(squares, axis=0)
        coarse = squares.astype(BF16)
        fine = (squares - coarse.astype(F32)).astype(BF16)
        sums = dot(jnp.concatenate([coarse, fine], axis=0), ones_bd)
        frob = jnp.sqrt(sums[:groups] + sums[groups:])
        inv_frob = 1.0 / frob
        scaling = jnp.sqrt((K - 1.0) * inv_frob)
        beta_all = 1.0 - shift * inv_frob
        batch = min(8, groups)
        for first in range(0, groups, batch):
            ids = range(first, first + batch)
            beta = [beta_all[g : g + 1] for g in ids]
            dev = [gs[g] * -inv_frob[g : g + 1] for g in ids]
            zeta = [1.0 + 0.5 * be for be in beta]
            root = [0.5 * d for d in dev]
            for it in range(ITERS):
                narrow = [d.astype(BF16) for d in dev]
                fixed = [block_diag(n) for n in narrow]
                if it == 0:
                    square = [dot(n, f) for n, f in zip(narrow, fixed)]
                elif it + 1 < ITERS:
                    both = [
                        dot(jnp.concatenate([n, r.astype(BF16)], axis=0), f)
                        for n, r, f in zip(narrow, root, fixed)
                    ]
                    square = [x[:K] for x in both]
                    prod = [x[K:] for x in both]
                else:
                    prod = [dot(r.astype(BF16), f) for r, f in zip(root, fixed)]
                if it > 0:
                    root = [
                        (1.0 + 0.5 * be) * r + (0.5 * ze) * d + 0.5 * x
                        for be, r, ze, d, x in zip(beta, root, zeta, dev, prod)
                    ]
                    zeta = [ze * (1.0 + 0.5 * be) for ze, be in zip(zeta, beta)]
                if it + 1 < ITERS:
                    square = [2.0 * be * d + s for be, d, s in zip(beta, dev, square)]
                    cube = [dot(s.astype(BF16), f) for s, f in zip(square, fixed)]
                    dev = [
                        (0.75 + 0.25 * be) * s + (0.25 * be * be) * d + 0.25 * c
                        for be, s, d, c in zip(beta, square, dev, cube)
                    ]
                    beta = [be * be * (0.75 + 0.25 * be) for be in beta]
            full = [ze * eye + r for ze, r in zip(zeta, root)]
            mean_row = []
            for g in ids:
                c0 = g * GROUP
                m = [mean_rows[c : c + 1] for c in range(c0, c0 + GROUP)]
                mean_row.append(
                    jnp.concatenate(
                        [jnp.where(low[:1], m[0], m[1]), jnp.where(low[:1], m[2], m[3])], axis=1
                    )
                )
            half_step = [
                ze * m
                + dot(
                    jnp.broadcast_to(m, (8, span)).astype(BF16), block_diag(r.astype(BF16))
                )[:1]
                for ze, m, r in zip(zeta, mean_row, root)
            ]
            shifted = [
                dot((f * h).astype(BF16), ones_bd) for f, h in zip(full, half_step)
            ]
            mix = []
            for f, ze, sh, g in zip(full, zeta, shifted, ids):
                scale = scaling[g : g + 1]
                mix.append(
                    (
                        scale * f
                        + (1.0 - scale * ze) * (1.0 / K)
                        + sh * inv_frob[g : g + 1]
                    ).astype(BF16)
                )
            applied = []
            for g, mx in zip(ids, mix):
                c0 = g * GROUP
                sides_in = []
                for c in (c0, c0 + 2):
                    here = xs[c * rows_x : (c + 1) * rows_x, :]
                    there = xs[(c + 1) * rows_x : (c + 2) * rows_x, :]
                    even = jnp.where(low_x, here, pltpu.roll(there, K, 1))
                    odd = jnp.where(low_x, pltpu.roll(here, K, 1), there)
                    sides_in.append(jnp.concatenate([even, odd], axis=0).astype(BF16))
                applied.append(dot(jnp.concatenate(sides_in, axis=1), block_diag(mx)))
            for g, result in zip(ids, applied):
                c0 = g * GROUP
                for side, c in enumerate((c0, c0 + 2)):
                    got = result[:, side * LANES : (side + 1) * LANES]
                    even, odd = got[:rows_x], got[rows_x:]
                    ys[c * rows_x : (c + 1) * rows_x, :] = jnp.where(low_x, even, pltpu.roll(odd, K, 1))
                    ys[(c + 1) * rows_x : (c + 2) * rows_x, :] = jnp.where(low_x, pltpu.roll(even, K, 1), odd)
        keep = lon * columns + iota((columns, LANES), 0) < count
        for p in range(pairs):
            out_ref[b, :, p * LANES : (p + 1) * LANES] = jnp.where(
                keep, ys[pl.ds(p, columns, stride=rows_x), :], 0.0
            ).astype(BF16)
        return carry

    lax.fori_loop(0, bands, one_band, 0)


def per_device(lats, lons, background, band_cols, obs_col, obs_lev, obs_mask, innov, obs_var):
    bands, columns, width = background.shape
    obs = obs_col.shape[1]
    pairs = width // LANES
    vmem = pl.BlockSpec(memory_space=pltpu.VMEM)
    smem = pl.BlockSpec(memory_space=pltpu.SMEM)
    dma = pltpu.SemaphoreType.DMA
    end_rows = bands * END_SLOTS // 2
    padded_pairs = -(-pairs // 8) * 8
    own, side, shift = pl.pallas_call(
        functools.partial(exchange_kernel, lats, lons),
        out_shape=(
            jax.ShapeDtypeStruct((bands * obs // 2, LANES), BF16),
            jax.ShapeDtypeStruct((3, end_rows, LANES), BF16),
            jax.ShapeDtypeStruct((8, LANES), F32),
        ),
        in_specs=[vmem] * 6 + [smem],
        out_specs=(vmem, vmem, vmem),
        scratch_shapes=[
            pltpu.VMEM((3, end_rows, LANES), BF16),
            pltpu.VMEM((3, end_rows, LANES), BF16),
            pltpu.VMEM((lons, end_rows, LANES), BF16),
            pltpu.VMEM((lats, 8, LANES), F32),
            pltpu.VMEM((lons, 8, LANES), F32),
            dma((2,)),
            dma((2,)),
            dma((lons,)),
            dma,
            dma,
            dma((lons,)),
            dma((lats,)),
            dma((lats,)),
            dma((lons,)),
            dma((lons,)),
        ],
        compiler_params=pltpu.CompilerParams(collective_id=0, has_side_effects=True),
        name="exchange",
    )(background, obs_col, obs_lev, obs_mask, innov, obs_var, band_cols)
    return pl.pallas_call(
        analysis_kernel,
        out_shape=jax.ShapeDtypeStruct(background.shape, BF16),
        in_specs=[vmem] * 5 + [smem],
        out_specs=vmem,
        scratch_shapes=[
            pltpu.VMEM((columns * padded_pairs, LANES), F32),
            pltpu.VMEM((columns * padded_pairs, LANES), F32),
            pltpu.VMEM((columns, 2 * LANES), F32),
            pltpu.VMEM((K, 2 * LANES), F32),
            pltpu.VMEM((2 * LANES, LANES), BF16),
            pltpu.VMEM((columns // GROUP, K, GROUP * K), F32),
        ],
        name="analysis",
    )(background, own, side, shift, obs_col, band_cols)


def solution(mesh):
    placed = (P("lat", "lon", None), P("lat")) + (P("lat", "lon"),) * 5
    return jax.shard_map(
        functools.partial(per_device, mesh.shape["lat"], mesh.shape["lon"]),
        mesh=mesh,
        in_specs=placed,
        out_specs=P("lat", "lon", None),
        check_vma=False,
    )
```
